32 devices in a mesh: sub: 8 (over z, y), leaf: 4 (over x, core).
Axes of the slice: x: 2, y: 2, z: 4, core: 2. Of those that a mesh axis runs over, the one named last changes fastest.
Arguments:
- child_row: int32 [16], P('sub'), may hold values from 0 to 15, each once
- counts: int32 [16], P('sub'), may hold values from 1 to 16, as said below
- live_mask: int32 [16, 16, 1326], P('sub', 'leaf'), may hold values 0 or 1
- hand_rank: int32 [16, 16, 1326], P('sub', 'leaf'), may hold values from 0 to 7461
- bet_size: float32 [16, 8], P('sub'), may hold values from 0.25 to 4
- pot_size: float32 [16], P('sub'), may hold values from 4 to 16
- trunk_ranges: float32 [16, 2, 1326], P('sub'), may hold values from 0.05 to 1
- trunk_values: float32 [16, 1326], P('sub'), may hold values from -8 to 8
Outputs:
- root_values: float32 [16, 2, 1326], P('sub')
The draws below stay inside these ranges and needn't reach their ends.
Inputs may be any that keep to these rules, and one draw needn't show every extreme that they name: Subgame s reads and returns row child_row[s] of the trunk's arrays; every row is named by exactly one subgame. Leaf blocks b < counts[s] of subgame s are used; some subgame uses all 16.
All inputs are finite; a program needn't handle non-finite values. No bound on the sum of `live_mask` on one device may be relied on, other than what follows from the above.
Results may differ from the reference program's by a relative error of at most 0.0004.
Values sent between devices are 32-bit elements; how exact they have to be, the bound alone decides.
A program may use at most 64 MiB of HBM per device.

```python
import math
import jax
import jax.numpy as jnp
from jax import lax

H = 1326
ACT = 8
ITERS = 4
S = 16
MAXB = 16


def draw_counts(key, part):
    key_one, key_two, key_three = jax.random.split(key, 3)
    first_draw = jax.random.randint(key_one, (S,), 1, MAXB + 1)
    second_draw = jax.random.randint(key_two, (S,), 1, MAXB + 1)
    picked = jnp.minimum(first_draw, second_draw)
    forced_at = jax.random.randint(key_three, (), 0, S)
    return jnp.where(jnp.arange(S) == forced_at, MAXB, picked).astype(jnp.int32)


def set_ends(array, key, smallest, high):
    extent = array.shape
    spot = [jax.random.randint(jax.random.fold_in(key, axis), (), 0, extent[axis]) for axis in range(len(extent))]
    array = array.at[tuple(spot)].set(smallest)
    longest = extent.index(max(extent))
    spot[longest] = (spot[longest] + 1) % extent[longest]
    return array.at[tuple(spot)].set(high)


def level_of(stream_key, extent, shards, low, high):
    factor_of = 1.0
    for dim, blocks in shards:
        heights = jax.random.uniform(jax.random.fold_in(jax.random.fold_in(stream_key, 6), dim), (blocks,), jnp.float32, low / len(shards), high / len(shards))
        factor_of = factor_of * jnp.repeat(jnp.exp(heights), extent[dim] // blocks).reshape((-1,) + (1,) * (len(extent) - 1 - dim))
    return factor_of


def normal_values(key, extent, width, limit, cuts=(), dtype=jnp.bfloat16):
    factor_of = level_of(key, extent, cuts, -0.22, 0.18) if cuts else 1.0
    result = jax.random.normal(key, extent, jnp.float32) * width * factor_of
    return jnp.minimum(jnp.maximum(result, -limit), limit).astype(dtype)


def setup_inputs(seed: int = 0) -> dict:
    key_list = jax.random.split(jax.random.key(seed), 9)
    child_row = jax.random.permutation(key_list[0], S).astype(jnp.int32)
    counts = draw_counts(jax.random.fold_in(key_list[8], 71), 0)
    live_mask = set_ends((jax.random.randint(key_list[2], (S, MAXB, H), 0, 8) < 7).astype(jnp.int32), jax.random.fold_in(key_list[2], 1), 0, 1)
    hand_rank = set_ends(jax.random.randint(key_list[3], (S, MAXB, H), 0, 7462), jax.random.fold_in(key_list[3], 1), 0, 7461).astype(jnp.int32)
    bet_size = jnp.clip(jnp.exp(math.log(4.0) - 2.7725887 * jax.random.uniform(key_list[4], (S, ACT), jnp.float32) ** level_of(key_list[4], (S, ACT), ((0, 8),), -0.2, 0.2)), 0.25, 4.0)
    pot_size = jnp.clip(jnp.exp(math.log(16.0) - 1.3862944 * jax.random.uniform(key_list[5], (S,), jnp.float32) ** level_of(key_list[5], (S,), ((0, 8),), -0.2, 0.2)), 4.0, 16.0)
    trunk_ranges = jnp.clip(jnp.exp(math.log(1.0) - 2.9957323 * jax.random.uniform(key_list[6], (S, 2, H), jnp.float32) ** level_of(key_list[6], (S, 2, H), ((0, 8),), -0.2, 0.2)), 0.05, 1.0)
    trunk_values = normal_values(key_list[7], (S, H), 1.5, 8.0, ((0, 8),), jnp.float32)
    return {"child_row": child_row, "counts": counts, "live_mask": live_mask, "hand_rank": hand_rank, "bet_size": bet_size, "pot_size": pot_size, "trunk_ranges": trunk_ranges, "trunk_values": trunk_values}


smooth = 0.1


def regret_match(positive, total_sum, option_count):
    return (positive + smooth) / (total_sum + option_count * smooth)


def solve_one(packed):
    used_count, live_slab, rank_slab, bet_row, pot_value, ranges, values = packed
    live_real = live_slab.astype(jnp.float32)
    block_ids = jnp.arange(MAXB)
    block_weight = jnp.where(block_ids < used_count, 1.0, 0.0).astype(jnp.float32) / used_count.astype(jnp.float32)
    sign_table = jnp.sign(rank_slab[:, :, None] - rank_slab[:, None, :]).astype(jnp.float32)
    showdown = sign_table * live_real[:, :, None] * live_real[:, None, :]
    own_range = ranges[0]
    opp_range = ranges[1]
    factor = pot_value * (1.0 + bet_row) / H
    regret_own = jnp.zeros((ACT, H), jnp.float32)
    call_regret = jnp.zeros((MAXB, ACT, H), jnp.float32)
    fold_regret = jnp.zeros((MAXB, ACT, H), jnp.float32)
    follow_regret = jnp.zeros((H,), jnp.float32)
    stop_regret = jnp.zeros((H,), jnp.float32)
    for step_index in range(ITERS):
        own_strategy = regret_match(regret_own, jnp.sum(regret_own, axis=0), ACT)
        call_prob = regret_match(call_regret, call_regret + fold_regret, 2)
        follow = regret_match(follow_regret, follow_regret + stop_regret, 2)
        reach_own = (own_range[None, :] * own_strategy).astype(jnp.bfloat16)
        entering = opp_range * follow
        reach_call = (entering[None, None, :] * call_prob).astype(jnp.bfloat16)
        reach_fold = entering[None, None, :] * (1.0 - call_prob)
        own_real = reach_own.astype(jnp.float32)
        columns = jnp.concatenate([reach_call.astype(jnp.float32), jnp.broadcast_to(own_real[None], (MAXB, ACT, H))], axis=1)
        applied = jnp.einsum('bij,bkj->bki', showdown, columns, precision=lax.Precision.HIGHEST)
        showdown_own = applied[:, :ACT]
        showdown_opp = applied[:, ACT:]
        fold_mass = jnp.sum(live_real[:, None, :] * reach_fold, axis=-1) / H
        own_mass = jnp.sum(live_real[:, None, :] * own_real[None], axis=-1) / H
        per_block = factor[None, :, None] * showdown_own + live_real[:, None, :] * (pot_value * fold_mass)[:, :, None]
        value_own = jnp.sum(block_weight[:, None, None] * per_block, axis=0)
        call_value = factor[None, :, None] * showdown_opp
        fold_value = -live_real[:, None, :] * (pot_value * own_mass)[:, :, None]
        node_value = call_prob * call_value + (1.0 - call_prob) * fold_value
        follow_value = jnp.sum(block_weight[:, None, None] * node_value, axis=(0, 1))
        gadget_value = follow * follow_value + (1.0 - follow) * values
        root_value = jnp.sum(own_strategy * value_own, axis=0)
        if step_index + 1 < ITERS:
            regret_own = jnp.maximum(regret_own + value_own - root_value[None, :], 0.0)
            call_regret = jnp.maximum(call_regret + call_value - node_value, 0.0)
            fold_regret = jnp.maximum(fold_regret + fold_value - node_value, 0.0)
            follow_regret = jnp.maximum(follow_regret + follow_value - gadget_value, 0.0)
            stop_regret = jnp.maximum(stop_regret + values - gadget_value, 0.0)
    return jnp.stack([root_value, jnp.maximum(values, follow_value)], axis=0)


def reference(child_row, counts, live_mask, hand_rank, bet_size, pot_size, trunk_ranges, trunk_values):
    gathered_ranges = trunk_ranges[child_row]
    gathered_values = trunk_values[child_row]
    results = lax.map(solve_one, (counts, live_mask, hand_rank, bet_size, pot_size, gathered_ranges, gathered_values))
    return jnp.zeros((S, 2, H), jnp.float32).at[child_row].set(results)
```

```python
import functools

import jax
import jax.numpy as jnp
from jax import lax
from jax.experimental import pallas as pl
from jax.experimental.pallas import tpu as pltpu
from jax.sharding import PartitionSpec as P

ACT = 8
ITERS = 4
smooth = 0.1
LANES = 128
ROWS = 32


def solve_kernel(
    subs, leaves, hands, wide, local, blocks,
    row_ref, count_ref, bet_ref, pot_ref, live_ref, rank_ref, range_ref, value_ref,
    out_ref,
    matrix, rank_pad, live, call_regret, fold_regret, regret_own, follow_regret, stop_regret,
    own_range, opp_range, values, strategy, follow, reach,
    sum_own, sum_follow, all_range, all_value, all_row, final,
    range_send, range_recv, value_send, value_recv, row_send, row_recv,
    own_send, own_recv, follow_send, follow_recv, final_send, final_recv,
):
    me = lax.axis_index("sub")
    leaf = lax.axis_index("leaf")
    f32 = jnp.float32

    barrier = pltpu.get_barrier_semaphore()

    def sub_peer(k):
        return lax.rem(me + k, subs)

    def greet(k, carry):
        pl.semaphore_signal(barrier, inc=1, device_id={"sub": sub_peer(k)}, device_id_type=pl.DeviceIdType.MESH)
        return carry

    lax.fori_loop(1, subs, greet, 0)
    leaf_peers = [lax.rem(leaf + k, leaves) for k in range(1, leaves)]
    for peer in leaf_peers:
        pl.semaphore_signal(barrier, inc=1, device_id={"leaf": peer}, device_id_type=pl.DeviceIdType.MESH)

    rank_pad[...] = jnp.zeros_like(rank_pad)
    live[...] = jnp.zeros_like(live)
    for s in range(local):
        rank_pad[s * blocks : (s + 1) * blocks, :hands] = rank_ref[s].astype(f32)
        for b in range(blocks):
            live[s * blocks + b, :, :hands] = jnp.broadcast_to(live_ref[s, b : b + 1].astype(f32), (ACT, hands))
        all_row[me, s : s + 1] = jnp.full((1, LANES), row_ref[s], jnp.int32)
    for ref in (call_regret, fold_regret, regret_own, follow_regret, stop_regret, own_range, opp_range, values):
        ref[...] = jnp.zeros_like(ref)

    rank_columns = rank_pad[...].T

    def build(block):
        matrix_rows = rank_pad[block : block + 1, :]

        for start in range(0, wide, ROWS):
            column = rank_columns[start : start + ROWS, block : block + 1]
            difference = matrix_rows - column
            matrix[block, start : start + ROWS, :] = jnp.clip(difference, -1.0, 1.0).astype(jnp.bfloat16)

    early = min(2, local * blocks)
    for block in range(early):
        build(block)

    pl.semaphore_wait(barrier, subs - 1 + leaves - 1)

    def gather_copies(k, source, target):
        here = pl.ds(source * local, local)
        to = {"sub": target}
        return (
            pltpu.make_async_remote_copy(
                src_ref=range_ref, dst_ref=all_range.at[here], send_sem=range_send.at[k], recv_sem=range_recv.at[source],
                device_id=to, device_id_type=pl.DeviceIdType.MESH),
            pltpu.make_async_remote_copy(
                src_ref=value_ref, dst_ref=all_value.at[source], send_sem=value_send.at[k], recv_sem=value_recv.at[source],
                device_id=to, device_id_type=pl.DeviceIdType.MESH),
            pltpu.make_async_remote_copy(
                src_ref=all_row.at[source], dst_ref=all_row.at[source], send_sem=row_send.at[k], recv_sem=row_recv.at[source],
                device_id=to, device_id_type=pl.DeviceIdType.MESH),
        )

    def gather_start(k, carry):
        for copy in gather_copies(k, me, sub_peer(k)):
            copy.start()
        return carry

    lax.fori_loop(1, subs, gather_start, 0)
    all_range[pl.ds(me * local, local)] = range_ref[...]
    all_value[me] = value_ref[...]

    for block in range(early, local * blocks):
        build(block)

    def gather_wait(k, carry):
        source = sub_peer(k)
        for copy in gather_copies(k, source, source):
            copy.wait_recv()
        for copy in gather_copies(k, me, source):
            copy.wait_send()
        return carry

    lax.fori_loop(1, subs, gather_wait, 0)

    act_index = lax.broadcasted_iota(jnp.int32, (ACT, wide), 0)
    for s in range(local):
        row = row_ref[s]
        picked = all_range[row]
        own_range[s, :, :hands] = picked[0:1]
        opp_range[s, :, :hands] = picked[1:2]
        values[s, :, :hands] = all_value[row // local, pl.ds(lax.rem(row, local), 1), :]

    def sum_copies(step, s, source, target):
        to = {"leaf": target}
        return (
            pltpu.make_async_remote_copy(
                src_ref=sum_own.at[step, s, source], dst_ref=sum_own.at[step, s, source],
                send_sem=own_send.at[step, s, target], recv_sem=own_recv.at[step, s, source],
                device_id=to, device_id_type=pl.DeviceIdType.MESH),
            pltpu.make_async_remote_copy(
                src_ref=sum_follow.at[step, s, source], dst_ref=sum_follow.at[step, s, source],
                send_sem=follow_send.at[step, s, target], recv_sem=follow_recv.at[step, s, source],
                device_id=to, device_id_type=pl.DeviceIdType.MESH),
        )

    def joined_sums(step, s):
        for peer in leaf_peers:
            for copy in sum_copies(step, s, peer, peer):
                copy.wait_recv()
        value_own = sum_own[step, s, 0]
        follow_value = sum_follow[step, s, 0]
        for index in range(1, leaves):
            value_own = value_own + sum_own[step, s, index]
            follow_value = follow_value + sum_follow[step, s, index]
        root_value = jnp.sum(strategy[s] * value_own, axis=0, keepdims=True)
        return value_own, follow_value, root_value

    def update(step, s):
        value_own, follow_value, root_value = joined_sums(step, s)
        gadget_value = follow[s] * follow_value + (1.0 - follow[s]) * values[s]
        regret_own[s] = jnp.maximum(regret_own[s] + value_own - root_value, 0.0)
        follow_regret[s] = jnp.maximum(follow_regret[s] + follow_value - gadget_value, 0.0)
        stop_regret[s] = jnp.maximum(stop_regret[s] + values[s] - gadget_value, 0.0)

    def sweep(step, s):
        own = regret_own[s]
        plan = (own + smooth) / (jnp.sum(own, axis=0, keepdims=True) + ACT * smooth)
        strategy[s] = plan
        enter = follow_regret[s]
        go = (enter + smooth) / (enter + stop_regret[s] + 2 * smooth)
        follow[s] = go
        reach[...] = (own_range[s] * plan).astype(jnp.bfloat16).astype(f32)
        entering = jnp.broadcast_to(opp_range[s] * go, (ACT, wide))
        pot = pot_ref[s]
        factor = jnp.zeros((ACT, wide), f32)
        for a in range(ACT):
            factor = jnp.where(act_index == a, pot * (1.0 + bet_ref[s, a]), factor)
        factor = factor / hands
        used = count_ref[s]
        share = 1.0 / jnp.full((1, wide), used.astype(f32), f32)

        def one_block(b, carry):
            part_own, part_follow = carry
            block = s * blocks + b
            mask = live[block]
            call = call_regret[block]
            fold = fold_regret[block]
            call_prob = (call + smooth) / (call + fold + 2 * smooth)
            stay = 1.0 - call_prob
            own_live = reach[...] * mask
            reach_call = ((entering * call_prob) * mask).astype(jnp.bfloat16)
            columns = jnp.concatenate([reach_call, own_live.astype(jnp.bfloat16)], axis=0)
            applied = jnp.dot(columns, matrix[block], preferred_element_type=f32)
            fold_mass = jnp.sum(mask * (entering * stay), axis=1, keepdims=True) / hands
            own_mass = jnp.sum(own_live, axis=1, keepdims=True) / hands
            scaled = factor * mask
            weight = share * jnp.where(leaf * blocks + b < used, 1.0, 0.0)
            part_own = part_own + weight * (scaled * applied[:ACT] + mask * (pot * fold_mass))
            call_value = scaled * applied[ACT:]
            fold_value = -mask * (pot * own_mass)
            node_value = call_prob * call_value + stay * fold_value
            part_follow = part_follow + weight * jnp.sum(node_value, axis=0, keepdims=True)
            call_regret[block] = jnp.maximum(call + call_value - node_value, 0.0)
            fold_regret[block] = jnp.maximum(fold + fold_value - node_value, 0.0)
            return part_own, part_follow

        part_own, part_follow = lax.fori_loop(
            0, blocks, one_block, (jnp.zeros((ACT, wide), f32), jnp.zeros((1, wide), f32)))
        sum_own[step, s, leaf] = part_own
        sum_follow[step, s, leaf] = part_follow
        for peer in leaf_peers:
            for copy in sum_copies(step, s, leaf, peer):
                copy.start()

    def iteration(step, carry):
        for s in range(local):
            @pl.when(step > 0)
            def _():
                update(step - 1, s)

            sweep(step, s)
        return carry

    lax.fori_loop(0, ITERS, iteration, 0)

    def final_copy(s, k, source, target):
        return pltpu.make_async_remote_copy(
            src_ref=final.at[source, s], dst_ref=final.at[source, s],
            send_sem=final_send.at[s, k], recv_sem=final_recv.at[s, source],
            device_id={"sub": target}, device_id_type=pl.DeviceIdType.MESH)

    for s in range(local):
        value_own, follow_value, root_value = joined_sums(ITERS - 1, s)
        final[me, s, 0:1] = root_value
        final[me, s, 1:2] = jnp.maximum(values[s], follow_value)

        def final_start(k, carry):
            final_copy(s, k, me, sub_peer(k)).start()
            return carry

        lax.fori_loop(1, subs, final_start, 0)

    def sums_sent(step, carry):
        for s in range(local):
            for peer in leaf_peers:
                for copy in sum_copies(step, s, leaf, peer):
                    copy.wait_send()
        return carry

    lax.fori_loop(0, ITERS, sums_sent, 0)

    def final_wait(k, carry):
        source = sub_peer(k)
        for s in range(local):
            final_copy(s, k, source, source).wait_recv()
            final_copy(s, k, me, source).wait_send()
        return carry

    lax.fori_loop(1, subs, final_wait, 0)

    def pick(source, rows):
        picked = list(rows)
        for s in range(local):
            named = all_row[source, s : s + 1, 0:1]
            result = final[source, s]
            for q in range(local):
                picked[q] = jnp.where(named == me * local + q, result, picked[q])
        return tuple(picked)

    rows = lax.fori_loop(0, subs, pick, tuple(jnp.zeros((2, wide), f32) for _ in range(local)))
    for q in range(local):
        out_ref[q] = rows[q][:, :hands]


def solution(mesh):
    subs = mesh.shape["sub"]
    leaves = mesh.shape["leaf"]

    def shards(child_row, counts, live_mask, hand_rank, bet_size, pot_size, trunk_ranges, trunk_values):
        local, blocks, hands = live_mask.shape
        wide = -(-hands // LANES) * LANES
        total = local * blocks
        f32 = jnp.float32
        smem = pl.BlockSpec(memory_space=pltpu.SMEM)
        vmem = pl.BlockSpec(memory_space=pltpu.VMEM)
        dma = pltpu.SemaphoreType.DMA
        scratch = [
            pltpu.VMEM((total, wide, wide), jnp.bfloat16),
            pltpu.VMEM((total, wide), f32),
            pltpu.VMEM((total, ACT, wide), f32),
            pltpu.VMEM((total, ACT, wide), f32),
            pltpu.VMEM((total, ACT, wide), f32),
            pltpu.VMEM((local, ACT, wide), f32),
            pltpu.VMEM((local, 1, wide), f32),
            pltpu.VMEM((local, 1, wide), f32),
            pltpu.VMEM((local, 1, wide), f32),
            pltpu.VMEM((local, 1, wide), f32),
            pltpu.VMEM((local, 1, wide), f32),
            pltpu.VMEM((local, ACT, wide), f32),
            pltpu.VMEM((local, 1, wide), f32),
            pltpu.VMEM((ACT, wide), f32),
            pltpu.VMEM((ITERS, local, leaves, ACT, wide), f32),
            pltpu.VMEM((ITERS, local, leaves, 1, wide), f32),
            pltpu.VMEM((subs * local, 2, hands), f32),
            pltpu.VMEM((subs, local, hands), f32),
            pltpu.VMEM((subs, local, LANES), jnp.int32),
            pltpu.VMEM((subs, local, 2, wide), f32),
        ]
        scratch += [dma((subs,))] * 6 + [dma((ITERS, local, leaves))] * 4 + [dma((local, subs))] * 2
        return pl.pallas_call(
            functools.partial(solve_kernel, subs, leaves, hands, wide, local, blocks),
            out_shape=jax.ShapeDtypeStruct((local, 2, hands), f32),
            in_specs=[smem, smem, smem, smem, vmem, vmem, vmem, vmem],
            out_specs=vmem,
            scratch_shapes=scratch,
            compiler_params=pltpu.CompilerParams(
                collective_id=0, has_side_effects=True, vmem_limit_bytes=60 * 1024 * 1024),
            name="gadget_sweep",
        )(child_row, counts, bet_size, pot_size, live_mask, hand_rank, trunk_ranges, trunk_values)

    in_specs = (
        P("sub"),
        P("sub"),
        P("sub", "leaf", None),
        P("sub", "leaf", None),
        P("sub", None),
        P("sub"),
        P("sub", None, None),
        P("sub", None),
    )
    return jax.shard_map(shards, mesh=mesh, in_specs=in_specs, out_specs=P("sub", None, None), check_vma=False)
```
